8 devices in a mesh: dp: 1 (over z), ep: 2 (over y), tp: 4 (over x, core).
Axes of the slice: x: 2, y: 2, z: 1, core: 2. Of those that a mesh axis runs over, the one named last changes fastest.
Arguments:
- x_in: bfloat16 [512, 1024], P(('dp', 'ep'))
- expert_ids: int32 [512, 8], P(('dp', 'ep'))
- gate_vals: float32 [512, 8], P(('dp', 'ep'))
- w_gate: bfloat16 [128, 1024, 1536], P('ep', None, 'tp')
- w_up: bfloat16 [128, 1024, 1536], P('ep', None, 'tp')
- w_down: bfloat16 [128, 1536, 1024], P('ep', 'tp')
Outputs:
- output: bfloat16 [512, 1024], P(('dp', 'ep'))
All inputs are finite; a program needn't handle non-finite values.
Results may differ from the reference program's by a relative error of at most 0.0101859.
Values are sent between devices in bfloat16 or wider.
A program may use at most 1 GiB of HBM per device.

```python
import jax
import jax.numpy as jnp
from jax import lax

D = 1024
FF = 1536
EXPERTS = 128
TOP = 8
TOKENS = 256
SOURCES = 2

CAPACITY = (5 * TOP * TOKENS) // (4 * EXPERTS)


def draw_routing(key, num_rows):
    scores = jax.random.randint(key, (num_rows, EXPERTS), 0, 1048576, dtype=jnp.int32)
    scores = scores * EXPERTS + jnp.arange(EXPERTS, dtype=jnp.int32)[None, :]
    _, chosen = lax.top_k(scores, TOP)
    return chosen.astype(jnp.int32)


def setup_inputs(seed: int = 0, part: int = 0) -> dict:
    base = jax.random.key(seed)
    key_x, key_ids, key_gate = jax.random.split(jax.random.fold_in(base, part), 3)
    key_wg, key_wu, key_wd = jax.random.split(jax.random.key(seed + 1), 3)
    num_rows = SOURCES * TOKENS
    x_in = jax.random.normal(key_x, (num_rows, D), jnp.float32).astype(jnp.bfloat16)
    expert_ids = draw_routing(key_ids, num_rows)
    gate_vals = jax.random.uniform(key_gate, (num_rows, TOP), jnp.float32, 0.25, 1.25)
    w_gate = (jax.random.normal(key_wg, (EXPERTS, D, FF), jnp.float32) * D ** -0.5).astype(jnp.bfloat16)
    w_up = (jax.random.normal(key_wu, (EXPERTS, D, FF), jnp.float32) * D ** -0.5).astype(jnp.bfloat16)
    w_down = (jax.random.normal(key_wd, (EXPERTS, FF, D), jnp.float32) * FF ** -0.5).astype(jnp.bfloat16)
    return {'x_in': x_in, 'expert_ids': expert_ids, 'gate_vals': gate_vals,
            'w_gate': w_gate, 'w_up': w_up, 'w_down': w_down}


def slot_numbers(ids_one):
    flat_ids = ids_one.reshape(TOKENS * TOP)
    onehot = (flat_ids[:, None] == jnp.arange(EXPERTS, dtype=jnp.int32)[None, :]).astype(jnp.int32)
    slots = jnp.sum((jnp.cumsum(onehot, axis=0) - onehot) * onehot, axis=1)
    return slots.reshape(TOKENS, TOP)


def reference(x_in, expert_ids, gate_vals, w_gate, w_up, w_down):
    x_src = x_in.reshape(SOURCES, TOKENS, D)
    ids_src = expert_ids.reshape(SOURCES, TOKENS, TOP)
    gates_src = gate_vals.reshape(SOURCES, TOKENS, TOP)
    slots = lax.map(slot_numbers, ids_src)
    kept = slots < CAPACITY
    flat_slot = jnp.where(kept, ids_src * CAPACITY + slots, EXPERTS * CAPACITY)
    token_num = jnp.broadcast_to(jnp.arange(TOKENS, dtype=jnp.int32)[:, None], (TOKENS, TOP))

    def dispatch(operands):
        tok_rows, slot_one = operands
        slot_owner = jnp.full((EXPERTS * CAPACITY + 1,), TOKENS, jnp.int32)
        slot_owner = slot_owner.at[slot_one.reshape(TOKENS * TOP)].set(token_num.reshape(TOKENS * TOP))
        padded = jnp.concatenate([tok_rows, jnp.zeros((1, D), tok_rows.dtype)], axis=0)
        return padded[slot_owner[: EXPERTS * CAPACITY]]

    slot_rows = lax.map(dispatch, (x_src, flat_slot))
    by_expert = slot_rows.reshape(SOURCES, EXPERTS, CAPACITY, D).transpose(1, 0, 2, 3)
    by_expert = by_expert.reshape(EXPERTS, SOURCES * CAPACITY, D)

    def expert_ffn(operands):
        rows_e, wg_e, wu_e, wd_e = operands
        gated = jax.nn.silu(jnp.dot(rows_e, wg_e, preferred_element_type=jnp.float32)) * jnp.dot(rows_e, wu_e, preferred_element_type=jnp.float32)
        hidden = gated.astype(jnp.bfloat16)
        return jnp.dot(hidden, wd_e, preferred_element_type=jnp.float32).astype(jnp.bfloat16)

    y_rows = lax.map(expert_ffn, (by_expert, w_gate, w_up, w_down))
    y_src = y_rows.reshape(EXPERTS, SOURCES, CAPACITY, D).transpose(1, 0, 2, 3)
    y_src = y_src.reshape(SOURCES, EXPERTS * CAPACITY, D)

    def combine(operands):
        y_one, slot_one, gate_one, kept_one = operands
        safe_slot = jnp.minimum(slot_one, EXPERTS * CAPACITY - 1)
        weight = jnp.where(kept_one, gate_one, 0.0)
        total = jnp.zeros((TOKENS, D), jnp.float32)
        for choice in range(TOP):
            total = total + weight[:, choice:choice + 1] * y_one[safe_slot[:, choice]].astype(jnp.float32)
        return total.astype(jnp.bfloat16)

    y_out = lax.map(combine, (y_src, flat_slot, gates_src, kept))
    return y_out.reshape(SOURCES * TOKENS, D)
```

```python
import functools

import jax
import jax.numpy as jnp
from jax import lax
from jax.experimental import pallas as pl
from jax.experimental.pallas import tpu as pltpu
from jax.sharding import PartitionSpec as P

CAP_NUM = 5
CAP_DEN = 4
GROUP = 4
SLOTS = 5
LAG = 3
FAR = -100.0

F32 = jnp.float32
BF16 = jnp.bfloat16


def moe_kernel(cap, x_hbm, ids_hbm, gates_hbm, wg_hbm, wu_hbm, wd_hbm, out_hbm,
               wgu, wd, x_own, x_oth, ids_v, gates_v, tr, r_own, r_out, r_in, r_oth, g_own,
               pbuf, d2d, qbuf, qrx, qry, qrd, acc, outb,
               w_sem, in_sem, xs_sem, xr_sem, rs_sem, ds_sem, dr_sem, qs_sem, qr_sem, as_sem, ar_sem, o_sem):
    n_loc, d_model, ff = wg_hbm.shape
    n_groups = n_loc // GROUP
    tokens, n_top = ids_hbm.shape
    n_exp = 2 * n_loc
    pad = 24
    pair_rows = 2 * cap
    rows = GROUP * cap

    ep = lax.axis_index("ep")
    tp = lax.axis_index("tp")
    core = lax.rem(tp, 2)
    xx = tp // 2
    sib = {"tp": xx * 2 + 1 - core}
    xpeer = {"tp": (1 - xx) * 2 + core}
    ypeer = {"ep": 1 - ep}
    diag = {"ep": 1 - ep, "tp": (1 - xx) * 2 + core}

    def remote(src, dst, ssem, rsem, dev):
        return pltpu.make_async_remote_copy(src_ref=src, dst_ref=dst, send_sem=ssem, recv_sem=rsem,
                                            device_id=dev, device_id_type=pl.DeviceIdType.MESH)

    def weights(g, slot):
        first = g * GROUP
        return (
            pltpu.make_async_copy(wg_hbm.at[pl.ds(first, GROUP)], wgu.at[slot, :, :, 0:ff], w_sem.at[slot, 0]),
            pltpu.make_async_copy(wu_hbm.at[pl.ds(first, GROUP)], wgu.at[slot, :, :, ff:2 * ff], w_sem.at[slot, 1]),
            pltpu.make_async_copy(wd_hbm.at[pl.ds(first, GROUP)], wd.at[slot], w_sem.at[slot, 2]),
        )

    ids_cp = pltpu.make_async_copy(ids_hbm, ids_v, in_sem.at[0])
    gates_cp = pltpu.make_async_copy(gates_hbm, gates_v, in_sem.at[1])
    x_cp = pltpu.make_async_copy(x_hbm, x_own, in_sem.at[2])
    ids_cp.start()
    gates_cp.start()
    x_cp.start()
    for s in range(SLOTS):
        for cp in weights(s, s):
            cp.start()

    barrier = pltpu.get_barrier_semaphore()
    for dev in (sib, xpeer, ypeer, diag):
        pl.semaphore_signal(barrier, inc=1, device_id=dev, device_id_type=pl.DeviceIdType.MESH)
    pl.semaphore_wait(barrier, 4)

    x_cp.wait()
    x_send = remote(x_own.at[core], x_oth.at[core], xs_sem.at[0], xr_sem.at[0], ypeer)
    x_send.start()

    ids_cp.wait()
    gates_cp.wait()
    tr[...] = jnp.zeros_like(tr)
    tr[:, 0:n_top] = ids_v[...].astype(F32)
    ids_t = tr[...].T
    tr[:, 0:n_top] = gates_v[...]
    gates_t = tr[...].T
    exp_id = lax.broadcasted_iota(jnp.int32, (n_exp, tokens), 0).astype(F32)
    member = jnp.zeros((n_exp, tokens), F32)
    gate = jnp.zeros((n_exp, tokens), F32)
    for j in range(n_top):
        hit = exp_id == ids_t[j:j + 1, :]
        member = jnp.where(hit, 1.0, member)
        gate = jnp.where(hit, gates_t[j:j + 1, :], gate)
    before = (lax.broadcasted_iota(jnp.int32, (tokens, tokens), 0)
              < lax.broadcasted_iota(jnp.int32, (tokens, tokens), 1))
    before = jnp.where(before, 1.0, 0.0).astype(BF16)
    rank = jnp.dot(member.astype(BF16), before, preferred_element_type=F32)
    kept = jnp.logical_and(member > 0.5, rank < cap - 0.5)
    slot_no = jnp.where(kept, rank, FAR)
    r_own[...] = slot_no.reshape(2, n_loc, tokens)
    r_out[...] = slot_no.astype(BF16).reshape(2, n_loc, tokens)
    g1 = gate.astype(BF16).astype(F32)
    g2 = (gate - g1).astype(BF16).astype(F32)
    g3 = gate - g1 - g2
    g_own[0] = g1.reshape(2, n_loc, tokens)
    g_own[1] = g2.reshape(2, n_loc, tokens)
    g_own[2] = g3.reshape(2, n_loc, tokens)
    acc[...] = jnp.zeros_like(acc)

    r_send = remote(r_out.at[1 - ep], r_in, rs_sem.at[0], rs_sem.at[1], ypeer)
    r_send.start()
    r_send.wait()
    r_oth[...] = r_in[...].astype(F32)

    x_send.wait()
    x_fwd = remote(x_oth.at[core], x_oth.at[core], xs_sem.at[1], xr_sem.at[1], sib)
    x_fwd.start()
    x_fwd.wait()

    row24 = lax.broadcasted_iota(jnp.int32, (pad, tokens), 0).astype(F32)

    def mask24(r_row, odd):
        return (row24 - 4.0 if odd else row24) == r_row

    def d2d_copy(g, slot):
        return remote(pbuf.at[slot, pl.ds(2 * (1 - core), 2)], d2d.at[g], ds_sem.at[slot], dr_sem.at[g], sib)

    def q_copies(g):
        return (
            remote(qbuf.at[g, 1 - xx, 0], qrx.at[g], qs_sem.at[0, g], qr_sem.at[0, g], xpeer),
            remote(qbuf.at[g, xx, 1], qry.at[g], qs_sem.at[1, g], qr_sem.at[1, g], ypeer),
            remote(qbuf.at[g, 1 - xx, 1], qrd.at[g], qs_sem.at[2, g], qr_sem.at[2, g], diag),
        )

    def matmuls(g):
        slot = lax.rem(g, SLOTS)
        ps = lax.rem(g, 2)
        for cp in weights(g, slot):
            cp.wait()

        @pl.when(g >= 2)
        def _():
            d2d_copy(g - 2, ps).wait_send()

        def pick(r_ref, x_ref):
            sel = jnp.concatenate(
                [jnp.where(mask24(r_ref[pl.ds(g * GROUP + i, 1), :], i % 2), 1.0, 0.0) for i in range(GROUP)], axis=0)
            return jnp.dot(sel.astype(BF16), x_ref[...].reshape(tokens, d_model), preferred_element_type=F32)

        own = pick(r_own.at[ep], x_own)
        oth = pick(r_oth, x_oth)
        res = []
        for i in range(GROUP):
            lhs = jnp.concatenate([own[pad * i:pad * (i + 1)], oth[pad * i:pad * (i + 1)]], axis=0).astype(BF16)
            gu = jnp.dot(lhs, wgu[slot, i], preferred_element_type=F32)
            hid = (jax.nn.silu(gu[:, 0:ff]) * gu[:, ff:2 * ff]).astype(BF16)
            res.append(jnp.dot(hid, wd[slot, i], preferred_element_type=F32))
            if i % 2 == 1:
                r0, r1 = res[i - 1], res[i]
                for src in range(2):
                    base = src * rows + (i // 2) * pair_rows
                    o = src * pad
                    for b in range(4):
                        cols = slice(b * 256, (b + 1) * 256)
                        pbuf[ps, b, base:base + 16, :] = r0[o:o + 16, cols]
                        pbuf[ps, b, base + 16:base + 24, :] = r0[o + 16:o + 24, cols] + r1[o:o + 8, cols]
                        pbuf[ps, b, base + 24:base + 40, :] = r1[o + 8:o + 24, cols]
        d2d_copy(g, ps).start()

        @pl.when(g + SLOTS < n_groups)
        def _():
            for cp in weights(g + SLOTS, slot):
                cp.start()

    def chip_sum(g):
        ps = lax.rem(g, 2)
        d2d_copy(g, ps).wait_recv()
        for xi in range(2):
            q = (pbuf[ps, 2 * core + xi] + d2d[g, xi]).astype(BF16)
            qbuf[g, xi] = q.reshape(2, rows, 256)
        for cp in q_copies(g):
            cp.start()

    def combine(g):
        for cp in q_copies(g):
            cp.wait()
        y_own = (qbuf[g, xx, 0].astype(F32) + qrx[g].astype(F32)).astype(BF16)
        y_oth = (qry[g].astype(F32) + qrd[g].astype(F32)).astype(BF16)
        lhs, rhs = [], []
        for side, y in ((ep, y_own), (1 - ep, y_oth)):
            masks = [mask24(r_own[side, pl.ds(g * GROUP + i, 1), :], i % 2) for i in range(GROUP)]
            for k in range(3):
                c = [jnp.where(masks[i], g_own[k, side, pl.ds(g * GROUP + i, 1), :], 0.0) for i in range(GROUP)]
                for p in range(GROUP // 2):
                    c0, c1 = c[2 * p], c[2 * p + 1]
                    lhs += [c0[0:16], c0[16:24] + c1[0:8], c1[8:24]]
                rhs.append(y)
        lhs = jnp.concatenate(lhs, axis=0).astype(BF16)
        rhs = jnp.concatenate(rhs, axis=0)
        acc[...] += lax.dot_general(lhs, rhs, (((0,), (0,)), ((), ())), preferred_element_type=F32)

    def step(g, carry):
        @pl.when(g < n_groups)
        def _():
            matmuls(g)

        @pl.when(jnp.logical_and(g >= 1, g < n_groups + 1))
        def _():
            chip_sum(g - 1)

        @pl.when(g >= LAG)
        def _():
            combine(g - LAG)

        return carry

    lax.fori_loop(0, n_groups + LAG, step, 0)
    for g in (n_groups - 2, n_groups - 1):
        d2d_copy(g, g % 2).wait_send()

    mine = 2 * core + xx
    outb[mine] = acc[...].astype(BF16)
    to_sib = remote(outb.at[mine], outb.at[mine], as_sem.at[0], ar_sem.at[0], sib)
    to_x = remote(outb.at[mine], outb.at[mine], as_sem.at[1], ar_sem.at[1], xpeer)
    to_x.start()
    to_sib.start()
    to_x.wait()
    far = 2 * core + 1 - xx
    fwd = remote(outb.at[far], outb.at[far], as_sem.at[2], ar_sem.at[2], sib)
    fwd.start()
    to_sib.wait()
    fwd.wait()
    outs = [pltpu.make_async_copy(outb.at[b], out_hbm.at[:, pl.ds(b * 256, 256)], o_sem.at[b]) for b in range(4)]
    for cp in outs:
        cp.start()
    for cp in outs:
        cp.wait()


def solution(mesh):
    row_spec = P(("dp", "ep"), None)

    def device_body(x_loc, ids_loc, gates_loc, wg_loc, wu_loc, wd_loc):
        tokens, d_model = x_loc.shape
        n_top = ids_loc.shape[1]
        n_loc, _, ff = wg_loc.shape
        n_exp = 2 * n_loc
        cap = CAP_NUM * n_top * tokens // (CAP_DEN * n_exp)
        rows = GROUP * cap
        n_groups = n_loc // GROUP
        dma = pltpu.SemaphoreType.DMA
        anys = pl.BlockSpec(memory_space=pl.ANY)
        return pl.pallas_call(
            functools.partial(moe_kernel, cap),
            out_shape=jax.ShapeDtypeStruct((tokens, d_model), BF16),
            in_specs=[anys] * 6,
            out_specs=anys,
            scratch_shapes=[
                pltpu.VMEM((SLOTS, GROUP, d_model, 2 * ff), BF16),
                pltpu.VMEM((SLOTS, GROUP, ff, d_model), BF16),
                pltpu.VMEM((2, tokens // 2, d_model), BF16),
                pltpu.VMEM((2, tokens // 2, d_model), BF16),
                pltpu.VMEM((tokens, n_top), jnp.int32),
                pltpu.VMEM((tokens, n_top), F32),
                pltpu.VMEM((tokens, 128), F32),
                pltpu.VMEM((2, n_loc, tokens), F32),
                pltpu.VMEM((2, n_loc, tokens), BF16),
                pltpu.VMEM((n_loc, tokens), BF16),
                pltpu.VMEM((n_loc, tokens), F32),
                pltpu.VMEM((3, 2, n_loc, tokens), F32),
                pltpu.VMEM((2, 4, 2 * rows, 256), F32),
                pltpu.VMEM((n_groups, 2, 2 * rows, 256), F32),
                pltpu.VMEM((n_groups, 2, 2, rows, 256), BF16),
                pltpu.VMEM((n_groups, rows, 256), BF16),
                pltpu.VMEM((n_groups, rows, 256), BF16),
                pltpu.VMEM((n_groups, rows, 256), BF16),
                pltpu.VMEM((tokens, 256), F32),
                pltpu.VMEM((4, tokens, 256), BF16),
                dma((SLOTS, 3)), dma((3,)), dma((2,)), dma((2,)), dma((2,)), dma((2,)), dma((n_groups,)),
                dma((3, n_groups)), dma((3, n_groups)), dma((3,)), dma((3,)), dma((4,)),
            ],
            compiler_params=pltpu.CompilerParams(
                collective_id=0, has_side_effects=True, vmem_limit_bytes=67043328),
        )(x_loc.reshape(2, tokens // 2, d_model), ids_loc, gates_loc, wg_loc, wu_loc, wd_loc)

    return jax.shard_map(device_body, mesh=mesh,
                         in_specs=(row_spec, row_spec, row_spec, P("ep", None, "tp"), P("ep", None, "tp"), P("ep", "tp", None)),
                         out_specs=row_spec, check_vma=False)
```

```python
import functools

import jax
import jax.numpy as jnp
from jax import lax
from jax.experimental import pallas as pl
from jax.experimental.pallas import tpu as pltpu
from jax.sharding import PartitionSpec as P

CAP_NUM = 5
CAP_DEN = 4
GROUP = 4
SLOTS = 5
LAG = 3
FAR = -100.0

F32 = jnp.float32
BF16 = jnp.bfloat16


def moe_kernel(cap, x_hbm, ids_hbm, gates_hbm, wg_hbm, wu_hbm, wd_hbm, out_hbm,
               wgu, wd, x_own, x_oth, ids_v, gates_v, r_own, r_out, r_in, r_oth, g_own, lhs_v,
               pbuf, d2d, qbuf, qrx, qry, qrd, acc, outb,
               w_sem, in_sem, xs_sem, xr_sem, rs_sem, ds_sem, dr_sem, qs_sem, qr_sem, as_sem, ar_sem, o_sem):
    n_loc, d_model, ff = wg_hbm.shape
    n_groups = n_loc // GROUP
    n_top, tokens = ids_hbm.shape
    n_exp = 2 * n_loc
    pad = 24
    pair_rows = 2 * cap
    rows = GROUP * cap

    ep = lax.axis_index("ep")
    tp = lax.axis_index("tp")
    core = lax.rem(tp, 2)
    xx = tp // 2
    sib = {"tp": xx * 2 + 1 - core}
    xpeer = {"tp": (1 - xx) * 2 + core}
    ypeer = {"ep": 1 - ep}
    diag = {"ep": 1 - ep, "tp": (1 - xx) * 2 + core}

    def remote(src, dst, ssem, rsem, dev):
        return pltpu.make_async_remote_copy(src_ref=src, dst_ref=dst, send_sem=ssem, recv_sem=rsem,
                                            device_id=dev, device_id_type=pl.DeviceIdType.MESH)

    def weights(g, slot):
        first = g * GROUP
        return (
            pltpu.make_async_copy(wg_hbm.at[pl.ds(first, GROUP)], wgu.at[slot, :, :, 0:ff], w_sem.at[slot, 0]),
            pltpu.make_async_copy(wu_hbm.at[pl.ds(first, GROUP)], wgu.at[slot, :, :, ff:2 * ff], w_sem.at[slot, 1]),
            pltpu.make_async_copy(wd_hbm.at[pl.ds(first, GROUP)], wd.at[slot], w_sem.at[slot, 2]),
        )

    ids_cp = pltpu.make_async_copy(ids_hbm, ids_v, in_sem.at[0])
    gates_cp = pltpu.make_async_copy(gates_hbm, gates_v, in_sem.at[1])
    x_cp = pltpu.make_async_copy(x_hbm, x_own, in_sem.at[2])
    ids_cp.start()
    gates_cp.start()
    x_cp.start()
    for s in range(SLOTS):
        for cp in weights(s, s):
            cp.start(priority=1)

    barrier = pltpu.get_barrier_semaphore()
    for dev in (sib, xpeer, ypeer, diag):
        pl.semaphore_signal(barrier, inc=1, device_id=dev, device_id_type=pl.DeviceIdType.MESH)
    pl.semaphore_wait(barrier, 4)

    x_cp.wait()
    x_send = remote(x_own.at[core], x_oth.at[core], xs_sem.at[0], xr_sem.at[0], ypeer)
    x_send.start()

    ids_cp.wait()
    gates_cp.wait()
    ids_t = ids_v[...].astype(F32)
    gates_t = gates_v[...]
    exp_id = lax.broadcasted_iota(jnp.int32, (n_exp, tokens), 0).astype(F32)
    member = jnp.zeros((n_exp, tokens), F32)
    gate = jnp.zeros((n_exp, tokens), F32)
    for j in range(n_top):
        hit = exp_id == ids_t[j:j + 1, :]
        member = jnp.where(hit, 1.0, member)
        gate = jnp.where(hit, gates_t[j:j + 1, :], gate)
    before = (lax.broadcasted_iota(jnp.int32, (tokens, tokens), 0)
              < lax.broadcasted_iota(jnp.int32, (tokens, tokens), 1))
    before = jnp.where(before, 1.0, 0.0).astype(BF16)
    rank = jnp.dot(member.astype(BF16), before, preferred_element_type=F32)
    kept = jnp.logical_and(member > 0.5, rank < cap - 0.5)
    slot_no = jnp.where(kept, rank, FAR)
    r_own[...] = slot_no.reshape(2, n_loc, tokens)
    r_out[...] = slot_no.astype(BF16).reshape(2, n_loc, tokens)
    g1 = gate.astype(BF16).astype(F32)
    g2 = (gate - g1).astype(BF16).astype(F32)
    g3 = gate - g1 - g2
    g_own[0] = g1.reshape(2, n_loc, tokens)
    g_own[1] = g2.reshape(2, n_loc, tokens)
    g_own[2] = g3.reshape(2, n_loc, tokens)
    acc[...] = jnp.zeros_like(acc)

    r_send = remote(r_out.at[1 - ep], r_in, rs_sem.at[0], rs_sem.at[1], ypeer)
    r_send.start()
    r_send.wait()
    r_oth[...] = r_in[...].astype(F32)

    x_send.wait()
    x_fwd = remote(x_oth.at[core], x_oth.at[core], xs_sem.at[1], xr_sem.at[1], sib)
    x_fwd.start()
    x_fwd.wait()

    row24 = lax.broadcasted_iota(jnp.int32, (pad, tokens), 0).astype(F32)

    def mask24(r_row, odd):
        return (row24 - 4.0 if odd else row24) == r_row

    def pick(g):
        both = []
        for r_ref, x_ref in ((r_own.at[ep], x_own), (r_oth, x_oth)):
            sel = jnp.concatenate(
                [jnp.where(mask24(r_ref[pl.ds(g * GROUP + i, 1), :], i % 2), 1.0, 0.0) for i in range(GROUP)], axis=0)
            both.append(jnp.dot(sel.astype(BF16), x_ref[...].reshape(tokens, d_model), preferred_element_type=F32))
        parts = [v[pad * i:pad * (i + 1)] for i in range(GROUP) for v in both]
        return jnp.concatenate(parts, axis=0).astype(BF16)

    def d2d_copy(g, slot):
        return remote(pbuf.at[slot, pl.ds(2 * (1 - core), 2)], d2d.at[g], ds_sem.at[slot], dr_sem.at[g], sib)

    def q_copies(g):
        return (
            remote(qbuf.at[g, 1 - xx, 0], qrx.at[g], qs_sem.at[0, g], qr_sem.at[0, g], xpeer),
            remote(qbuf.at[g, xx, 1], qry.at[g], qs_sem.at[1, g], qr_sem.at[1, g], ypeer),
            remote(qbuf.at[g, 1 - xx, 1], qrd.at[g], qs_sem.at[2, g], qr_sem.at[2, g], diag),
        )

    def matmuls(g):
        slot = lax.rem(g, SLOTS)
        ps = lax.rem(g, 2)
        for cp in weights(g, slot):
            cp.wait()

        @pl.when(g >= 2)
        def _():
            d2d_copy(g - 2, ps).wait_send()

        def up(i):
            return jnp.dot(lhs_v[pad * 2 * i:pad * 2 * (i + 1), :], wgu[slot, i], preferred_element_type=F32)

        def down(gu, i):
            hid = (jax.nn.silu(gu[:, 0:ff]) * gu[:, ff:2 * ff]).astype(BF16)
            return jnp.dot(hid, wd[slot, i], preferred_element_type=F32)

        gu = [up(0)]
        res = []
        for i in range(GROUP):
            if i + 1 < GROUP:
                gu.append(up(i + 1))
            else:
                nxt = pick(jnp.minimum(g + 1, n_groups - 1))
            res.append(down(gu[i], i))
            if i % 2 == 1:
                r0, r1 = res[i - 1], res[i]
                for src in range(2):
                    base = src * rows + (i // 2) * pair_rows
                    o = src * pad
                    for b in range(4):
                        cols = slice(b * 256, (b + 1) * 256)
                        pbuf[ps, b, base:base + 16, :] = r0[o:o + 16, cols]
                        pbuf[ps, b, base + 16:base + 24, :] = r0[o + 16:o + 24, cols] + r1[o:o + 8, cols]
                        pbuf[ps, b, base + 24:base + 40, :] = r1[o + 8:o + 24, cols]
        lhs_v[...] = nxt
        d2d_copy(g, ps).start()

        @pl.when(g + SLOTS < n_groups)
        def _():
            for cp in weights(g + SLOTS, slot):
                cp.start(priority=1)

    def chip_sum(g):
        ps = lax.rem(g, 2)
        d2d_copy(g, ps).wait_recv()
        for xi in range(2):
            q = (pbuf[ps, 2 * core + xi] + d2d[g, xi]).astype(BF16)
            qbuf[g, xi] = q.reshape(2, rows, 256)
        for cp in q_copies(g):
            cp.start()

    def combine(g):
        for cp in q_copies(g):
            cp.wait()
        y_own = (qbuf[g, xx, 0].astype(F32) + qrx[g].astype(F32)).astype(BF16)
        y_oth = (qry[g].astype(F32) + qrd[g].astype(F32)).astype(BF16)
        lhs, rhs = [], []
        for side, y in ((ep, y_own), (1 - ep, y_oth)):
            masks = [mask24(r_own[side, pl.ds(g * GROUP + i, 1), :], i % 2) for i in range(GROUP)]
            for k in range(3):
                c = [jnp.where(masks[i], g_own[k, side, pl.ds(g * GROUP + i, 1), :], 0.0) for i in range(GROUP)]
                for p in range(GROUP // 2):
                    c0, c1 = c[2 * p], c[2 * p + 1]
                    lhs += [c0[0:16], c0[16:24] + c1[0:8], c1[8:24]]
                rhs.append(y)
        lhs = jnp.concatenate(lhs, axis=0).astype(BF16)
        rhs = jnp.concatenate(rhs, axis=0)
        acc[...] += lax.dot_general(lhs, rhs, (((0,), (0,)), ((), ())), preferred_element_type=F32)

    lhs_v[...] = pick(0)

    def step(g, carry):
        @pl.when(g < n_groups)
        def _():
            matmuls(g)

        @pl.when(jnp.logical_and(g >= 1, g < n_groups + 1))
        def _():
            chip_sum(g - 1)

        @pl.when(g >= LAG)
        def _():
            combine(g - LAG)

        return carry

    lax.fori_loop(0, n_groups + LAG, step, 0)
    for g in (n_groups - 2, n_groups - 1):
        d2d_copy(g, g % 2).wait_send()

    mine = 2 * core + xx
    outb[mine] = acc[...].astype(BF16)
    to_sib = remote(outb.at[mine], outb.at[mine], as_sem.at[0], ar_sem.at[0], sib)
    to_x = remote(outb.at[mine], outb.at[mine], as_sem.at[1], ar_sem.at[1], xpeer)
    to_x.start()
    to_sib.start()
    to_x.wait()
    far = 2 * core + 1 - xx
    fwd = remote(outb.at[far], outb.at[far], as_sem.at[2], ar_sem.at[2], sib)
    fwd.start()
    to_sib.wait()
    fwd.wait()
    outs = [pltpu.make_async_copy(outb.at[b], out_hbm.at[:, pl.ds(b * 256, 256)], o_sem.at[b]) for b in range(4)]
    for cp in outs:
        cp.start()
    for cp in outs:
        cp.wait()


def solution(mesh):
    row_spec = P(("dp", "ep"), None)

    def device_body(x_loc, ids_loc, gates_loc, wg_loc, wu_loc, wd_loc):
        tokens, d_model = x_loc.shape
        n_top = ids_loc.shape[1]
        n_loc, _, ff = wg_loc.shape
        n_exp = 2 * n_loc
        cap = CAP_NUM * n_top * tokens // (CAP_DEN * n_exp)
        rows = GROUP * cap
        n_groups = n_loc // GROUP
        dma = pltpu.SemaphoreType.DMA
        anys = pl.BlockSpec(memory_space=pl.ANY)
        return pl.pallas_call(
            functools.partial(moe_kernel, cap),
            out_shape=jax.ShapeDtypeStruct((tokens, d_model), BF16),
            in_specs=[anys] * 6,
            out_specs=anys,
            scratch_shapes=[
                pltpu.VMEM((SLOTS, GROUP, d_model, 2 * ff), BF16),
                pltpu.VMEM((SLOTS, GROUP, ff, d_model), BF16),
                pltpu.VMEM((2, tokens // 2, d_model), BF16),
                pltpu.VMEM((2, tokens // 2, d_model), BF16),
                pltpu.VMEM((n_top, tokens), jnp.int32),
                pltpu.VMEM((n_top, tokens), F32),
                pltpu.VMEM((2, n_loc, tokens), F32),
                pltpu.VMEM((2, n_loc, tokens), BF16),
                pltpu.VMEM((n_loc, tokens), BF16),
                pltpu.VMEM((n_loc, tokens), F32),
                pltpu.VMEM((3, 2, n_loc, tokens), F32),
                pltpu.VMEM((GROUP * 48, d_model), BF16),
                pltpu.VMEM((2, 4, 2 * rows, 256), F32),
                pltpu.VMEM((n_groups, 2, 2 * rows, 256), F32),
                pltpu.VMEM((n_groups, 2, 2, rows, 256), BF16),
                pltpu.VMEM((n_groups, rows, 256), BF16),
                pltpu.VMEM((n_groups, rows, 256), BF16),
                pltpu.VMEM((n_groups, rows, 256), BF16),
                pltpu.VMEM((tokens, 256), F32),
                pltpu.VMEM((4, tokens, 256), BF16),
                dma((SLOTS, 3)), dma((3,)), dma((2,)), dma((2,)), dma((2,)), dma((2,)), dma((n_groups,)),
                dma((3, n_groups)), dma((3, n_groups)), dma((3,)), dma((3,)), dma((4,)),
            ],
            compiler_params=pltpu.CompilerParams(
                collective_id=0, has_side_effects=True, vmem_limit_bytes=67043328),
        )(x_loc.reshape(2, tokens // 2, d_model), ids_loc.T, gates_loc.T, wg_loc, wu_loc, wd_loc)

    return jax.shard_map(device_body, mesh=mesh,
                         in_specs=(row_spec, row_spec, row_spec, P("ep", None, "tp"), P("ep", None, "tp"), P("ep", "tp", None)),
                         out_specs=row_spec, check_vma=False)
```

```python
import functools

import jax
import jax.numpy as jnp
from jax import lax
from jax.experimental import pallas as pl
from jax.experimental.pallas import tpu as pltpu
from jax.sharding import PartitionSpec as P

CAP_NUM = 5
CAP_DEN = 4
PAIRS = 2
SLOTS = 10
TAIL = 4
LAG = 4
FAR = -100.0

F32 = jnp.float32
BF16 = jnp.bfloat16


def moe_kernel(cap, x_hbm, ids_hbm, gates_hbm, wg_hbm, wu_hbm, wd_hbm, out_hbm,
               wgu, wd, x_own, x_oth, ids_v, gates_v, r_own, r_out, r_in, r_oth, g_own, lhs_v,
               pbuf, d2d, qbuf, qrx, qry, qrd, acc,
               w_sem, in_sem, xs_sem, xr_sem, rs_sem, ds_sem, dr_sem, qs_sem, qr_sem, as_sem, ar_sem):
    n_loc, d_model, ff = wg_hbm.shape
    n_pairs = n_loc // 2
    n_main = (n_pairs - TAIL) // PAIRS
    n_units = n_main + TAIL
    n_top, tokens = ids_hbm.shape
    n_exp = 2 * n_loc
    pad = 24
    pair_rows = 2 * cap

    ep = lax.axis_index("ep")
    tp = lax.axis_index("tp")
    core = lax.rem(tp, 2)
    xx = tp // 2
    sib = {"tp": xx * 2 + 1 - core}
    xpeer = {"tp": (1 - xx) * 2 + core}
    ypeer = {"ep": 1 - ep}
    diag = {"ep": 1 - ep, "tp": (1 - xx) * 2 + core}

    def remote(src, dst, ssem, rsem, dev):
        return pltpu.make_async_remote_copy(src_ref=src, dst_ref=dst, send_sem=ssem, recv_sem=rsem,
                                            device_id=dev, device_id_type=pl.DeviceIdType.MESH)

    def weights(p):
        slot = lax.rem(p, SLOTS)
        two = pl.ds(2 * p, 2)
        return (
            pltpu.make_async_copy(wg_hbm.at[two], wgu.at[slot, :, :, 0:ff], w_sem.at[slot, 0]),
            pltpu.make_async_copy(wu_hbm.at[two], wgu.at[slot, :, :, ff:2 * ff], w_sem.at[slot, 1]),
            pltpu.make_async_copy(wd_hbm.at[two], wd.at[slot], w_sem.at[slot, 2]),
        )

    def start_weights(p):
        for cp in weights(p):
            cp.start(priority=1)

    ids_cp = pltpu.make_async_copy(ids_hbm, ids_v, in_sem.at[0])
    gates_cp = pltpu.make_async_copy(gates_hbm, gates_v, in_sem.at[1])
    x_cp = pltpu.make_async_copy(x_hbm, x_own, in_sem.at[2])
    ids_cp.start()
    gates_cp.start()
    x_cp.start()
    for p in range(SLOTS):
        start_weights(p)

    barrier = pltpu.get_barrier_semaphore()
    for dev in (sib, xpeer, ypeer, diag):
        pl.semaphore_signal(barrier, inc=1, device_id=dev, device_id_type=pl.DeviceIdType.MESH)
    pl.semaphore_wait(barrier, 4)

    x_cp.wait()
    x_send = remote(x_own.at[core], x_oth.at[core], xs_sem.at[0], xr_sem.at[0], ypeer)
    x_send.start()

    ids_cp.wait()
    gates_cp.wait()
    ids_t = ids_v[...].astype(F32)
    gates_t = gates_v[...]
    exp_id = lax.broadcasted_iota(jnp.int32, (n_exp, tokens), 0).astype(F32)
    member = jnp.zeros((n_exp, tokens), F32)
    gate = jnp.zeros((n_exp, tokens), F32)
    for j in range(n_top):
        hit = exp_id == ids_t[j:j + 1, :]
        member = jnp.where(hit, 1.0, member)
        gate = jnp.where(hit, gates_t[j:j + 1, :], gate)
    before = (lax.broadcasted_iota(jnp.int32, (tokens, tokens), 0)
              < lax.broadcasted_iota(jnp.int32, (tokens, tokens), 1))
    before = jnp.where(before, 1.0, 0.0).astype(BF16)
    rank = jnp.dot(member.astype(BF16), before, preferred_element_type=F32)
    kept = jnp.logical_and(member > 0.5, rank < cap - 0.5)
    slot_no = jnp.where(kept, rank, FAR)
    r_own[...] = slot_no.reshape(2, n_loc, tokens)
    r_out[...] = slot_no.astype(BF16).reshape(2, n_loc, tokens)
    g1 = gate.astype(BF16).astype(F32)
    g2 = (gate - g1).astype(BF16).astype(F32)
    g3 = gate - g1 - g2
    g_own[0] = g1.reshape(2, n_loc, tokens)
    g_own[1] = g2.reshape(2, n_loc, tokens)
    g_own[2] = g3.reshape(2, n_loc, tokens)
    acc[...] = jnp.zeros_like(acc)

    r_send = remote(r_out.at[1 - ep], r_in, rs_sem.at[0], rs_sem.at[1], ypeer)
    r_send.start()
    r_send.wait()
    r_oth[...] = r_in[...].astype(F32)

    x_send.wait()
    x_fwd = remote(x_oth.at[core], x_oth.at[core], xs_sem.at[1], xr_sem.at[1], sib)
    x_fwd.start()
    x_fwd.wait()

    row24 = lax.broadcasted_iota(jnp.int32, (pad, tokens), 0).astype(F32)

    def mask24(r_row, odd):
        return (row24 - 4.0 if odd else row24) == r_row

    def pick(p0):
        both = []
        for r_ref, x_ref in ((r_own.at[ep], x_own), (r_oth, x_oth)):
            sel = jnp.concatenate(
                [jnp.where(mask24(r_ref[pl.ds(2 * p0 + i, 1), :], i % 2), 1.0, 0.0) for i in range(2 * PAIRS)], axis=0)
            both.append(jnp.dot(sel.astype(BF16), x_ref[...].reshape(tokens, d_model), preferred_element_type=F32))
        parts = [v[pad * i:pad * (i + 1)] for i in range(2 * PAIRS) for v in both]
        return jnp.concatenate(parts, axis=0).astype(BF16)

    def d2d_copy(unit):
        u, p0, n = unit
        slot = lax.rem(u, 2)
        return remote(pbuf.at[slot, pl.ds(0, n), pl.ds(2 * (1 - core), 2)], d2d.at[pl.ds(p0, n)],
                      ds_sem.at[slot], dr_sem.at[u], sib)

    def q_copies(unit):
        u, p0, n = unit
        ps = pl.ds(p0, n)
        return (
            remote(qbuf.at[1 - xx, 0, ps], qrx.at[ps], qs_sem.at[0, u], qr_sem.at[0, u], xpeer),
            remote(qbuf.at[xx, 1, ps], qry.at[ps], qs_sem.at[1, u], qr_sem.at[1, u], ypeer),
            remote(qbuf.at[1 - xx, 1, ps], qrd.at[ps], qs_sem.at[2, u], qr_sem.at[2, u], diag),
        )

    def matmuls(unit, lhs0, nxt_pair, split):
        u, p0, n = unit
        ps = lax.rem(u, 2)
        cps = [weights(p0 + i) for i in range(n)]
        for cp in cps:
            cp[0].wait()
            cp[1].wait()
        if not split:
            for cp in cps:
                cp[2].wait()
        slots = [lax.rem(p0 + i, SLOTS) for i in range(n)]

        def up(i):
            lhs = lhs_v[lhs0 + 2 * pad * i:lhs0 + 2 * pad * (i + 1), :]
            return jnp.dot(lhs, wgu[slots[i // 2], i % 2], preferred_element_type=F32)

        def act(gu):
            return (jax.nn.silu(gu[:, 0:ff]) * gu[:, ff:2 * ff]).astype(BF16)

        def down(hid, i):
            return jnp.dot(hid, wd[slots[i // 2], i % 2], preferred_element_type=F32)

        def put(i, r0, r1):
            for src in range(2):
                base = src * pair_rows
                o = src * pad
                for b in range(4):
                    cols = slice(b * 256, (b + 1) * 256)
                    pbuf[ps, i, b, base:base + 16, :] = r0[o:o + 16, cols]
                    pbuf[ps, i, b, base + 16:base + 24, :] = r0[o + 16:o + 24, cols] + r1[o:o + 8, cols]
                    pbuf[ps, i, b, base + 24:base + 40, :] = r1[o + 8:o + 24, cols]

        nxt = None
        if split:
            hids = [act(g) for g in [up(i) for i in range(2 * n)]]
            for cp in cps:
                cp[2].wait()
            res = [down(h, i) for i, h in enumerate(hids)]
            for i in range(n):
                put(i, res[2 * i], res[2 * i + 1])
        else:
            gu = [up(0)]
            res = []
            for i in range(2 * n):
                if i + 1 < 2 * n:
                    gu.append(up(i + 1))
                elif nxt_pair is not None:
                    nxt = pick(nxt_pair)
                res.append(down(act(gu[i]), i))
                if i % 2 == 1:
                    put(i // 2, res[i - 1], res[i])
        if nxt is not None:
            lhs_v[...] = nxt
        d2d_copy(unit).start()

    def chip_sum(unit):
        u, p0, n = unit
        ps = lax.rem(u, 2)
        d2d_copy(unit).wait_recv()
        for i in range(n):
            for xi in range(2):
                q = (pbuf[ps, i, 2 * core + xi] + d2d[p0 + i, xi]).astype(BF16)
                qbuf[xi, 0, p0 + i] = q[0:pair_rows]
                qbuf[xi, 1, p0 + i] = q[pair_rows:2 * pair_rows]
        for cp in q_copies(unit):
            cp.start()

    def combine(unit):
        u, p0, n = unit
        for cp in q_copies(unit):
            cp.wait()
        lhs, rhs = [], []
        for here in (True, False):
            side = ep if here else 1 - ep
            y = []
            for i in range(n):
                if here:
                    parts = qbuf[xx, 0, p0 + i], qrx[p0 + i]
                else:
                    parts = qry[p0 + i], qrd[p0 + i]
                y.append(parts[0].astype(F32) + parts[1].astype(F32))
            for k in range(3):
                for i in range(n):
                    c = []
                    for odd in range(2):
                        e = pl.ds(2 * (p0 + i) + odd, 1)
                        c.append(jnp.where(mask24(r_own[side, e, :], odd), g_own[k, side, e, :], 0.0))
                    lhs += [c[0][0:16], c[0][16:24] + c[1][0:8], c[1][8:24]]
                    rhs.append(y[i])
        lhs = jnp.concatenate(lhs, axis=0).astype(BF16)
        rhs = jnp.concatenate(rhs, axis=0).astype(BF16)
        acc[...] += lax.dot_general(lhs, rhs, (((0,), (0,)), ((), ())), preferred_element_type=F32)

    def main_unit(u):
        return u, PAIRS * u, PAIRS

    lhs_v[...] = pick(0)

    def step(u, carry):
        @pl.when(u >= 2)
        def _():
            d2d_copy(main_unit(u - 2)).wait_send()

        matmuls(main_unit(u), 0, PAIRS * (u + 1), False)
        for i in range(PAIRS):
            p = PAIRS * u + i + SLOTS

            @pl.when(p < n_pairs)
            def _():
                start_weights(p)

        @pl.when(u >= 1)
        def _():
            chip_sum(main_unit(u - 1))

        @pl.when(u >= LAG)
        def _():
            combine(main_unit(u - LAG))

        return carry

    lax.fori_loop(0, n_main, step, 0)

    units = [main_unit(u) for u in range(n_main)]
    units += [(n_main + t, n_main * PAIRS + t, 1) for t in range(TAIL)]
    for t in range(TAIL):
        u = n_main + t
        last = t == TAIL - 1
        d2d_copy(units[u - 2]).wait_send()
        nxt_pair = units[u][1] + 1 if t % 2 == 1 and not last else None
        matmuls(units[u], 2 * 2 * pad * (t % 2), nxt_pair, False)
        chip_sum(units[u - 1])
    chip_sum(units[n_units - 1])
    for u in range(n_main - LAG, n_units):
        combine(units[u])
    for u in range(n_units - 2, n_units):
        d2d_copy(units[u]).wait_send()

    mine = 2 * core + xx

    def blk(b):
        return out_hbm.at[:, pl.ds(pl.multiple_of(b * 256, 256), 256)]

    out_hbm[:, pl.ds(pl.multiple_of(mine * 256, 256), 256)] = acc[...].astype(BF16)
    to_sib = remote(blk(mine), blk(mine), as_sem.at[0], ar_sem.at[0], sib)
    to_x = remote(blk(mine), blk(mine), as_sem.at[1], ar_sem.at[1], xpeer)
    to_x.start()
    to_sib.start()
    to_x.wait()
    far = 2 * core + 1 - xx
    fwd = remote(blk(far), blk(far), as_sem.at[2], ar_sem.at[2], sib)
    fwd.start()
    to_sib.wait()
    fwd.wait()


def solution(mesh):
    row_spec = P(("dp", "ep"), None)

    def device_body(x_loc, ids_loc, gates_loc, wg_loc, wu_loc, wd_loc):
        tokens, d_model = x_loc.shape
        n_top = ids_loc.shape[1]
        n_loc, _, ff = wg_loc.shape
        n_exp = 2 * n_loc
        cap = CAP_NUM * n_top * tokens // (CAP_DEN * n_exp)
        rows = 2 * cap
        n_pairs = n_loc // 2
        n_units = (n_pairs - TAIL) // PAIRS + TAIL
        dma = pltpu.SemaphoreType.DMA
        anys = pl.BlockSpec(memory_space=pl.ANY)
        return pl.pallas_call(
            functools.partial(moe_kernel, cap),
            out_shape=pltpu.VMEM((tokens, d_model), BF16),
            in_specs=[anys] * 6,
            out_specs=pl.BlockSpec(memory_space=pltpu.VMEM),
            scratch_shapes=[
                pltpu.VMEM((SLOTS, 2, d_model, 2 * ff), BF16),
                pltpu.VMEM((SLOTS, 2, ff, d_model), BF16),
                pltpu.VMEM((2, tokens // 2, d_model), BF16),
                pltpu.VMEM((2, tokens // 2, d_model), BF16),
                pltpu.VMEM((n_top, tokens), jnp.int32),
                pltpu.VMEM((n_top, tokens), F32),
                pltpu.VMEM((2, n_loc, tokens), F32),
                pltpu.VMEM((2, n_loc, tokens), BF16),
                pltpu.VMEM((n_loc, tokens), BF16),
                pltpu.VMEM((n_loc, tokens), F32),
                pltpu.VMEM((3, 2, n_loc, tokens), F32),
                pltpu.VMEM((PAIRS * 2 * 48, d_model), BF16),
                pltpu.VMEM((2, PAIRS, 4, 2 * rows, 256), F32),
                pltpu.VMEM((n_pairs, 2, 2 * rows, 256), F32),
                pltpu.VMEM((2, 2, n_pairs, rows, 256), BF16),
                pltpu.VMEM((n_pairs, rows, 256), BF16),
                pltpu.VMEM((n_pairs, rows, 256), BF16),
                pltpu.VMEM((n_pairs, rows, 256), BF16),
                pltpu.VMEM((tokens, 256), F32),
                dma((SLOTS, 3)), dma((3,)), dma((2,)), dma((2,)), dma((2,)), dma((2,)), dma((n_units,)),
                dma((3, n_units)), dma((3, n_units)), dma((3,)), dma((3,)),
            ],
            compiler_params=pltpu.CompilerParams(
                collective_id=0, has_side_effects=True, vmem_limit_bytes=63 * 1024 * 1024),
        )(x_loc.reshape(2, tokens // 2, d_model), ids_loc.T, gates_loc.T, wg_loc, wu_loc, wd_loc)

    return jax.shard_map(device_body, mesh=mesh,
                         in_specs=(row_spec, row_spec, row_spec, P("ep", None, "tp"), P("ep", None, "tp"), P("ep", "tp", None)),
                         out_specs=row_spec, check_vma=False)
```

```python
import functools

import jax
import jax.numpy as jnp
from jax import lax
from jax.experimental import pallas as pl
from jax.experimental.pallas import tpu as pltpu
from jax.sharding import PartitionSpec as P

CAP_NUM = 5
CAP_DEN = 4
PAIRS = 2
SLOTS = 10
TAIL = 4
LAG = 4
FAR = -100.0

F32 = jnp.float32
BF16 = jnp.bfloat16


def moe_kernel(cap, x_hbm, ids_hbm, gates_hbm, wg_hbm, wu_hbm, wd_hbm, out_hbm,
               wgu, wd, x_own, x_oth, ids_v, gates_v, r_own, r_out, r_in, r_oth, g_own, lhs_v,
               pbuf, d2d, qbuf, qrx, qry, qrd, acc,
               w_sem, in_sem, xs_sem, xr_sem, rs_sem, ds_sem, dr_sem, qs_sem, qr_sem, as_sem, ar_sem):
    n_loc, d_model, ff = wg_hbm.shape
    n_pairs = n_loc // 2
    n_main = (n_pairs - TAIL) // PAIRS
    n_units = n_main + TAIL
    n_top, tokens = ids_hbm.shape
    n_exp = 2 * n_loc
    pad = 24
    pair_rows = 2 * cap

    ep = lax.axis_index("ep")
    tp = lax.axis_index("tp")
    core = lax.rem(tp, 2)
    xx = tp // 2
    sib = {"tp": xx * 2 + 1 - core}
    xpeer = {"tp": (1 - xx) * 2 + core}
    ypeer = {"ep": 1 - ep}
    diag = {"ep": 1 - ep, "tp": (1 - xx) * 2 + core}

    def remote(src, dst, ssem, rsem, dev):
        return pltpu.make_async_remote_copy(src_ref=src, dst_ref=dst, send_sem=ssem, recv_sem=rsem,
                                            device_id=dev, device_id_type=pl.DeviceIdType.MESH)

    def weights(p):
        slot = lax.rem(p, SLOTS)
        two = pl.ds(2 * p, 2)
        return (
            pltpu.make_async_copy(wg_hbm.at[two], wgu.at[slot, :, :, 0:ff], w_sem.at[slot, 0]),
            pltpu.make_async_copy(wu_hbm.at[two], wgu.at[slot, :, :, ff:2 * ff], w_sem.at[slot, 1]),
            pltpu.make_async_copy(wd_hbm.at[two], wd.at[slot], w_sem.at[slot, 2]),
        )

    def start_weights(p):
        for cp in weights(p):
            cp.start(priority=1)

    ids_cp = pltpu.make_async_copy(ids_hbm, ids_v, in_sem.at[0])
    gates_cp = pltpu.make_async_copy(gates_hbm, gates_v, in_sem.at[1])
    x_cp = pltpu.make_async_copy(x_hbm, x_own, in_sem.at[2])
    ids_cp.start()
    gates_cp.start()
    x_cp.start()
    for p in range(SLOTS):
        start_weights(p)

    barrier = pltpu.get_barrier_semaphore()
    for dev in (sib, xpeer, ypeer, diag):
        pl.semaphore_signal(barrier, inc=1, device_id=dev, device_id_type=pl.DeviceIdType.MESH)
    pl.semaphore_wait(barrier, 4)

    x_cp.wait()
    x_send = remote(x_own.at[core], x_oth.at[core], xs_sem.at[0], xr_sem.at[0], ypeer)
    x_send.start()

    ids_cp.wait()
    gates_cp.wait()
    ids_t = ids_v[...].astype(F32)
    gates_t = gates_v[...]
    exp_id = lax.broadcasted_iota(jnp.int32, (n_exp, tokens), 0).astype(F32)
    member = jnp.zeros((n_exp, tokens), F32)
    gate = jnp.zeros((n_exp, tokens), F32)
    for j in range(n_top):
        hit = exp_id == ids_t[j:j + 1, :]
        member = jnp.where(hit, 1.0, member)
        gate = jnp.where(hit, gates_t[j:j + 1, :], gate)
    before = (lax.broadcasted_iota(jnp.int32, (tokens, tokens), 0)
              < lax.broadcasted_iota(jnp.int32, (tokens, tokens), 1))
    before = jnp.where(before, 1.0, 0.0).astype(BF16)
    rank = jnp.dot(member.astype(BF16), before, preferred_element_type=F32)
    kept = jnp.logical_and(member > 0.5, rank < cap - 0.5)
    slot_no = jnp.where(kept, rank, FAR)
    r_own[...] = slot_no.reshape(2, n_loc, tokens)
    r_out[...] = slot_no.astype(BF16).reshape(2, n_loc, tokens)
    g1 = gate.astype(BF16).astype(F32)
    g2 = (gate - g1).astype(BF16).astype(F32)
    g3 = gate - g1 - g2
    g_own[0] = g1.reshape(2, n_loc, tokens)
    g_own[1] = g2.reshape(2, n_loc, tokens)
    g_own[2] = g3.reshape(2, n_loc, tokens)
    acc[...] = jnp.zeros_like(acc)

    r_send = remote(r_out.at[1 - ep], r_in, rs_sem.at[0], rs_sem.at[1], ypeer)
    r_send.start()
    r_send.wait()
    r_oth[...] = r_in[...].astype(F32)

    x_send.wait()
    x_fwd = remote(x_oth.at[core], x_oth.at[core], xs_sem.at[1], xr_sem.at[1], sib)
    x_fwd.start()
    x_fwd.wait()

    row24 = lax.broadcasted_iota(jnp.int32, (pad, tokens), 0).astype(F32)

    def mask24(r_row, odd):
        return (row24 - 4.0 if odd else row24) == r_row

    def pick(p0):
        both = []
        for r_ref, x_ref in ((r_own.at[ep], x_own), (r_oth, x_oth)):
            sel = jnp.concatenate(
                [jnp.where(mask24(r_ref[pl.ds(2 * p0 + i, 1), :], i % 2), 1.0, 0.0) for i in range(2 * PAIRS)], axis=0)
            both.append(jnp.dot(sel.astype(BF16), x_ref[...].reshape(tokens, d_model), preferred_element_type=F32))
        parts = [v[pad * i:pad * (i + 1)] for i in range(2 * PAIRS) for v in both]
        return jnp.concatenate(parts, axis=0).astype(BF16)

    def d2d_copy(unit):
        u, p0, n = unit
        slot = lax.rem(u, 2)
        return remote(pbuf.at[slot, pl.ds(0, n), pl.ds(2 * (1 - core), 2)], d2d.at[pl.ds(p0, n)],
                      ds_sem.at[slot], dr_sem.at[u], sib)

    def q_copies(unit):
        u, p0, n = unit
        ps = pl.ds(p0, n)
        return (
            remote(qbuf.at[1 - xx, 0, ps], qrx.at[ps], qs_sem.at[0, u], qr_sem.at[0, u], xpeer),
            remote(qbuf.at[xx, 1, ps], qry.at[ps], qs_sem.at[1, u], qr_sem.at[1, u], ypeer),
            remote(qbuf.at[1 - xx, 1, ps], qrd.at[ps], qs_sem.at[2, u], qr_sem.at[2, u], diag),
        )

    def matmuls(unit, lhs0, nxt_pair, split):
        u, p0, n = unit
        ps = lax.rem(u, 2)
        cps = [weights(p0 + i) for i in range(n)]
        for cp in cps:
            cp[0].wait()
            cp[1].wait()
        if not split:
            for cp in cps:
                cp[2].wait()
        slots = [lax.rem(p0 + i, SLOTS) for i in range(n)]

        def up(i):
            lhs = lhs_v[lhs0 + 2 * pad * i:lhs0 + 2 * pad * (i + 1), :]
            return jnp.dot(lhs, wgu[slots[i // 2], i % 2], preferred_element_type=F32)

        def act(gu):
            return (jax.nn.silu(gu[:, 0:ff]) * gu[:, ff:2 * ff]).astype(BF16)

        def down(hid, i):
            return jnp.dot(hid, wd[slots[i // 2], i % 2], preferred_element_type=F32)

        def put(i, r0, r1):
            for src in range(2):
                base = src * pair_rows
                o = src * pad
                for b in range(4):
                    cols = slice(b * 256, (b + 1) * 256)
                    pbuf[ps, i, b, base:base + 16, :] = r0[o:o + 16, cols]
                    pbuf[ps, i, b, base + 16:base + 24, :] = r0[o + 16:o + 24, cols] + r1[o:o + 8, cols]
                    pbuf[ps, i, b, base + 24:base + 40, :] = r1[o + 8:o + 24, cols]

        nxt = None
        if split:
            hids = [act(g) for g in [up(i) for i in range(2 * n)]]
            for cp in cps:
                cp[2].wait()
            res = [down(h, i) for i, h in enumerate(hids)]
            for i in range(n):
                put(i, res[2 * i], res[2 * i + 1])
        else:
            gu = [up(0)]
            res = []
            for i in range(2 * n):
                if i + 1 < 2 * n:
                    gu.append(up(i + 1))
                elif nxt_pair is not None:
                    nxt = pick(nxt_pair)
                res.append(down(act(gu[i]), i))
                if i % 2 == 1:
                    put(i // 2, res[i - 1], res[i])
        if nxt is not None:
            lhs_v[...] = nxt
        d2d_copy(unit).start()

    def chip_sum(unit):
        u, p0, n = unit
        ps = lax.rem(u, 2)
        d2d_copy(unit).wait_recv()
        for i in range(n):
            for xi in range(2):
                q = (pbuf[ps, i, 2 * core + xi] + d2d[p0 + i, xi]).astype(BF16)
                qbuf[xi, 0, p0 + i] = q[0:pair_rows]
                qbuf[xi, 1, p0 + i] = q[pair_rows:2 * pair_rows]
        for cp in q_copies(unit):
            cp.start()

    def combine(unit):
        u, p0, n = unit
        for cp in q_copies(unit):
            cp.wait()
        lhs, rhs = [], []
        for here in (True, False):
            side = ep if here else 1 - ep
            y = []
            for i in range(n):
                if here:
                    parts = qbuf[xx, 0, p0 + i], qrx[p0 + i]
                else:
                    parts = qry[p0 + i], qrd[p0 + i]
                y.append(parts[0].astype(F32) + parts[1].astype(F32))
            for k in range(3):
                for i in range(n):
                    c = []
                    for odd in range(2):
                        e = pl.ds(2 * (p0 + i) + odd, 1)
                        c.append(jnp.where(mask24(r_own[side, e, :], odd), g_own[k, side, e, :], 0.0))
                    lhs += [c[0][0:16], c[0][16:24] + c[1][0:8], c[1][8:24]]
                    rhs.append(y[i])
        lhs = jnp.concatenate(lhs, axis=0).astype(BF16)
        rhs = jnp.concatenate(rhs, axis=0).astype(BF16)
        acc[...] += lax.dot_general(lhs, rhs, (((0,), (0,)), ((), ())), preferred_element_type=F32)

    def main_unit(u):
        return u, PAIRS * u, PAIRS

    lhs_v[...] = pick(0)

    def step(u, carry):
        @pl.when(u >= 2)
        def _():
            d2d_copy(main_unit(u - 2)).wait_send()

        matmuls(main_unit(u), 0, PAIRS * (u + 1), False)
        for i in range(PAIRS):
            p = PAIRS * u + i + SLOTS

            @pl.when(p < n_pairs)
            def _():
                start_weights(p)

        @pl.when(u >= 1)
        def _():
            chip_sum(main_unit(u - 1))

        @pl.when(u >= LAG)
        def _():
            combine(main_unit(u - LAG))

        return carry

    lax.fori_loop(0, n_main, step, 0)

    units = [main_unit(u) for u in range(n_main)]
    units += [(n_main + t, n_main * PAIRS + t, 1) for t in range(TAIL)]
    for t in range(TAIL):
        u = n_main + t
        last = t == TAIL - 1
        d2d_copy(units[u - 2]).wait_send()
        nxt_pair = units[u][1] + 1 if t % 2 == 1 and not last else None
        matmuls(units[u], 2 * 2 * pad * (t % 2), nxt_pair, False)
        chip_sum(units[u - 1])
    chip_sum(units[n_units - 1])
    for u in range(n_main - LAG, n_units):
        combine(units[u])
    for u in range(n_units - 2, n_units):
        d2d_copy(units[u]).wait_send()

    def share(r0, r1, sem, dev, block):
        ref = out_hbm.at[pl.ds(r0, r1 - r0), pl.ds(pl.multiple_of(block * 256, 256), 256)]
        return remote(ref, ref, as_sem.at[sem], ar_sem.at[sem], dev)

    mine, other = 2 * core + xx, 2 * core + 1 - xx
    third = tokens - 16
    mid = tokens // 2
    out_hbm[:, pl.ds(pl.multiple_of(mine * 256, 256), 256)] = acc[...].astype(BF16)
    x1 = share(0, mid, 0, xpeer, mine)
    s1 = share(0, tokens, 1, sib, mine)
    x2 = share(mid, third, 2, xpeer, mine)
    x3 = share(third, tokens, 3, xpeer, mine)
    x1.start()
    x2.start()
    x3.start()
    s1.start()
    x1.wait()
    f1 = share(0, mid, 5, sib, other)
    f1.start()
    x2.wait()
    f2 = share(mid, third, 6, sib, other)
    f2.start()
    x3.wait()
    f3 = share(third, tokens, 4, sib, other)
    f3.start()
    for cp in (s1, f1, f2, f3):
        cp.wait()


def solution(mesh):
    row_spec = P(("dp", "ep"), None)

    def device_body(x_loc, ids_loc, gates_loc, wg_loc, wu_loc, wd_loc):
        tokens, d_model = x_loc.shape
        n_top = ids_loc.shape[1]
        n_loc, _, ff = wg_loc.shape
        n_exp = 2 * n_loc
        cap = CAP_NUM * n_top * tokens // (CAP_DEN * n_exp)
        rows = 2 * cap
        n_pairs = n_loc // 2
        n_units = (n_pairs - TAIL) // PAIRS + TAIL
        dma = pltpu.SemaphoreType.DMA
        anys = pl.BlockSpec(memory_space=pl.ANY)
        return pl.pallas_call(
            functools.partial(moe_kernel, cap),
            out_shape=pltpu.VMEM((tokens, d_model), BF16),
            in_specs=[anys] * 6,
            out_specs=pl.BlockSpec(memory_space=pltpu.VMEM),
            scratch_shapes=[
                pltpu.VMEM((SLOTS, 2, d_model, 2 * ff), BF16),
                pltpu.VMEM((SLOTS, 2, ff, d_model), BF16),
                pltpu.VMEM((2, tokens // 2, d_model), BF16),
                pltpu.VMEM((2, tokens // 2, d_model), BF16),
                pltpu.VMEM((n_top, tokens), jnp.int32),
                pltpu.VMEM((n_top, tokens), F32),
                pltpu.VMEM((2, n_loc, tokens), F32),
                pltpu.VMEM((2, n_loc, tokens), BF16),
                pltpu.VMEM((n_loc, tokens), BF16),
                pltpu.VMEM((n_loc, tokens), F32),
                pltpu.VMEM((3, 2, n_loc, tokens), F32),
                pltpu.VMEM((PAIRS * 2 * 48, d_model), BF16),
                pltpu.VMEM((2, PAIRS, 4, 2 * rows, 256), F32),
                pltpu.VMEM((n_pairs, 2, 2 * rows, 256), F32),
                pltpu.VMEM((2, 2, n_pairs, rows, 256), BF16),
                pltpu.VMEM((n_pairs, rows, 256), BF16),
                pltpu.VMEM((n_pairs, rows, 256), BF16),
                pltpu.VMEM((n_pairs, rows, 256), BF16),
                pltpu.VMEM((tokens, 256), F32),
                dma((SLOTS, 3)), dma((3,)), dma((2,)), dma((2,)), dma((2,)), dma((2,)), dma((n_units,)),
                dma((3, n_units)), dma((3, n_units)), dma((8,)), dma((8,)),
            ],
            compiler_params=pltpu.CompilerParams(
                collective_id=0, has_side_effects=True, vmem_limit_bytes=63 * 1024 * 1024),
        )(x_loc.reshape(2, tokens // 2, d_model), ids_loc.T, gates_loc.T, wg_loc, wu_loc, wd_loc)

    return jax.shard_map(device_body, mesh=mesh,
                         in_specs=(row_spec, row_spec, row_spec, P("ep", None, "tp"), P("ep", None, "tp"), P("ep", "tp", None)),
                         out_specs=row_spec, check_vma=False)
```
